16 devices in a mesh: batch: 2 (over y, z), dap: 8 (over x, core).
Axes of the slice: x: 4, y: 2, z: 1, core: 2. Of those that a mesh axis runs over, the one named last changes fastest.
The devices are a block of a 4x4x8 slice.
Arguments:
- pair_act: bfloat16 [768, 384, 128], P(('batch', 'dap')), parts along dimension 0
- pair_mask: int32 [768, 384], P(('batch', 'dap')), parts along dimension 0
- ln_in_scale: bfloat16 [2, 128], replicated
- ln_in_bias: bfloat16 [2, 128], replicated
- w_in: bfloat16 [2, 128, 512], replicated
- b_in: bfloat16 [2, 512], replicated
- w_gate: bfloat16 [2, 128, 128], replicated
- b_gate: bfloat16 [2, 128], replicated
- ln_out_scale: bfloat16 [2, 128], replicated
- ln_out_bias: bfloat16 [2, 128], replicated
- w_out: bfloat16 [2, 128, 128], replicated
- b_out: bfloat16 [2, 128], replicated
Outputs:
- output: bfloat16 [768, 384, 128], P(('batch', 'dap')), parts along dimension 0
There are 2 independent parts. The reference program is written for one: setup_inputs(seed, part) draws one part's arguments, and reference() takes and returns one part's arrays. A program takes and returns all parts, laid end to end along the dimension named above; an argument that names none is the same for every part.
All inputs are finite; a program needn't handle non-finite values.
Results may differ from the reference program's by a relative error of at most 0.00746292.
Values are sent between devices in bfloat16 or wider.
A program may use at most 768 MiB of HBM per device.

```python
import jax
import jax.numpy as jnp
from jax import lax

CZ = 128
CH = 128
N_RES = 384
ROW_BLOCK = 64
LAYERS = 2
LN_EPS = 1e-5


def setup_inputs(seed: int = 0, part: int = 0) -> dict:
    part_keys = jax.random.split(jax.random.fold_in(jax.random.key(seed), part), 2)
    shared_keys = jax.random.split(jax.random.key(seed + 1), 10)

    def draw_normal(key_index, shape, scale):
        return scale * jax.random.normal(shared_keys[key_index], shape, jnp.float32)

    pair_act = jax.random.normal(part_keys[0], (N_RES, N_RES, CZ), jnp.float32)
    mask_draw = jax.random.randint(part_keys[1], (N_RES, N_RES), 0, 10)
    pair_mask = (mask_draw >= 2).astype(jnp.int32)
    return {
        'pair_act': pair_act.astype(jnp.bfloat16),
        'pair_mask': pair_mask,
        'ln_in_scale': (1.0 + draw_normal(0, (LAYERS, CZ), 0.3)).astype(jnp.bfloat16),
        'ln_in_bias': draw_normal(1, (LAYERS, CZ), 0.3).astype(jnp.bfloat16),
        'w_in': draw_normal(2, (LAYERS, CZ, 4 * CH), CZ ** -0.5).astype(jnp.bfloat16),
        'b_in': draw_normal(3, (LAYERS, 4 * CH), 0.5).astype(jnp.bfloat16),
        'w_gate': draw_normal(4, (LAYERS, CZ, CZ), CZ ** -0.5).astype(jnp.bfloat16),
        'b_gate': draw_normal(5, (LAYERS, CZ), 0.5).astype(jnp.bfloat16),
        'ln_out_scale': (1.0 + draw_normal(6, (LAYERS, CH), 0.3)).astype(jnp.bfloat16),
        'ln_out_bias': draw_normal(7, (LAYERS, CH), 0.3).astype(jnp.bfloat16),
        'w_out': draw_normal(8, (LAYERS, CH, CZ), CH ** -0.5).astype(jnp.bfloat16),
        'b_out': draw_normal(9, (LAYERS, CZ), 0.3).astype(jnp.bfloat16),
    }


def layer_norm(values, ln_scale, offset):
    values = values.astype(jnp.float32)
    mean_val = jnp.mean(values, axis=-1, keepdims=True)
    centred = values - mean_val
    var_val = jnp.mean(centred * centred, axis=-1, keepdims=True)
    return centred * lax.rsqrt(var_val + LN_EPS) * ln_scale.astype(jnp.float32) + offset.astype(jnp.float32)


def gated_side(z_norm, mask_rows, w_pair, b_pair):
    projected = jnp.dot(z_norm.reshape(-1, CZ), w_pair, preferred_element_type=jnp.float32) + b_pair.astype(jnp.float32)
    gated = jax.nn.sigmoid(projected[:, CH:]) * projected[:, :CH] * mask_rows.reshape(-1, 1)
    return gated.astype(jnp.bfloat16).reshape(ROW_BLOCK, N_RES, CH)


def tri_update(z_cur, mask_f, layer_params):
    ln_in_s, ln_in_b, w_in_l, b_in_l, w_gate_l, b_gate_l, ln_out_s, ln_out_b, w_out_l, b_out_l = layer_params
    num_blocks = N_RES // ROW_BLOCK
    z_blocks = z_cur.reshape(num_blocks, ROW_BLOCK, N_RES, CZ)
    mask_blocks = mask_f.reshape(num_blocks, ROW_BLOCK, N_RES)

    def b_rows(block):
        z_rows, mask_rows = block
        z_norm = layer_norm(z_rows, ln_in_s, ln_in_b).astype(jnp.bfloat16)
        return gated_side(z_norm, mask_rows, w_in_l[:, 2 * CH:], b_in_l[2 * CH:])

    b_side = lax.map(b_rows, (z_blocks, mask_blocks)).reshape(N_RES, N_RES, CH).astype(jnp.float32)

    def out_rows(block):
        z_rows, mask_rows = block
        z_norm = layer_norm(z_rows, ln_in_s, ln_in_b).astype(jnp.bfloat16)
        a_side = gated_side(z_norm, mask_rows, w_in_l[:, :2 * CH], b_in_l[:2 * CH])
        tri_sum = jnp.einsum('ikc,jkc->ijc', a_side.astype(jnp.float32), b_side)
        o_norm = layer_norm(tri_sum, ln_out_s, ln_out_b).astype(jnp.bfloat16)
        update = jnp.dot(o_norm.reshape(-1, CH), w_out_l, preferred_element_type=jnp.float32) + b_out_l.astype(jnp.float32)
        update = update.astype(jnp.bfloat16).astype(jnp.float32)
        gate_val = jax.nn.sigmoid(jnp.dot(z_norm.reshape(-1, CZ), w_gate_l, preferred_element_type=jnp.float32) + b_gate_l.astype(jnp.float32))
        z_new = z_rows.reshape(-1, CZ).astype(jnp.float32) + gate_val * update
        return z_new.astype(jnp.bfloat16).reshape(ROW_BLOCK, N_RES, CZ)

    return lax.map(out_rows, (z_blocks, mask_blocks)).reshape(N_RES, N_RES, CZ)


def reference(pair_act, pair_mask, ln_in_scale, ln_in_bias, w_in, b_in, w_gate, b_gate, ln_out_scale, ln_out_bias, w_out, b_out):
    mask_f = pair_mask.astype(jnp.float32)

    def layer_step(z_cur, layer_params):
        return tri_update(z_cur, mask_f, layer_params), None

    stacked = (ln_in_scale, ln_in_bias, w_in, b_in, w_gate, b_gate, ln_out_scale, ln_out_bias, w_out, b_out)
    z_out, scan_tail = lax.scan(layer_step, pair_act, stacked)
    return z_out
```

```python
import functools

import jax
import jax.numpy as jnp
from jax import lax
from jax.experimental import pallas as pl
from jax.experimental.pallas import tpu as pltpu
from jax.sharding import PartitionSpec as P

LN_EPS = 1e-5
F32 = jnp.float32
BF = jnp.bfloat16
RB = 16
LANES = 128


def norm_columns(x, scale, bias):
    inv = 1.0 / x.shape[0]
    cen = x - jnp.sum(x, axis=0, keepdims=True) * inv
    var = jnp.sum(cen * cen, axis=0, keepdims=True) * inv
    return (cen * lax.rsqrt(var + LN_EPS) * scale + bias).astype(BF)


def proj_kernel(sides, pieces, want_zn, pos_ref, *refs):
    z_refs, refs = refs[:pieces], refs[pieces:]
    m_ref, s_ref, b_ref, w_ref = refs[:4]
    outs, refs = refs[4:4 + sides], refs[4 + sides:]
    if want_zn:
        zn_ref, refs = refs[0], refs[1:]
    znm, tmp = refs[0], refs[1]
    rows, width, d = z_refs[0].shape
    n, ka = znm.shape[2], znm.shape[1]
    if pieces > 1:
        zfull = refs[2]
        for q in range(pieces):
            zfull[:, pl.ds(pl.multiple_of(pos_ref[q] * width, RB), width), :] = z_refs[q][...]
    else:
        zfull = z_refs[0]
    ones_row = lax.broadcasted_iota(jnp.int32, (ka - d, LANES), 0) == 0
    unroll = 4

    @pl.loop(0, rows, step=unroll)
    def _(i0):
        for u in range(unroll):
            i = i0 + u
            m = m_ref[pl.ds(i, 1), :]
            for t in range(n // LANES):
                sl = slice(t * LANES, (t + 1) * LANES)
                y = norm_columns(zfull[i, sl, :].T.astype(F32), s_ref[...], b_ref[...])
                if want_zn:
                    zn_ref[i, sl, :] = y.T
                znm[i, :d, sl] = y * m[:, sl].astype(BF)
                znm[i, d:, sl] = jnp.where(ones_row, jnp.broadcast_to(m[:, sl], ones_row.shape), 0.0).astype(BF)

    parts, half = w_ref.shape[1], w_ref.shape[2] // 2

    @pl.loop(0, rows)
    def _(i):
        rhs = znm[i]
        for sd in range(sides):
            for h in range(parts):
                p = jnp.dot(w_ref[sd, h], rhs, preferred_element_type=F32)
                tmp[sd, i, h * half:(h + 1) * half, :] = (jax.nn.sigmoid(p[half:]) * p[:half]).astype(BF)

    @pl.loop(0, parts * half // RB)
    def _(k):
        k0 = pl.multiple_of(k * RB, RB)
        for sd in range(sides):
            outs[sd][pl.ds(k0, RB)] = jnp.transpose(tmp[sd, :, pl.ds(k0, RB), :], (1, 0, 2))


def project(zs, pos, mask, scale, bias, w, want_zn):
    r, width, d = zs[0].shape
    n = mask.shape[1]
    sides, parts, half2, ka = w.shape
    c = parts * half2 // 2
    out_shape = [jax.ShapeDtypeStruct((c, r, n), BF)] * sides
    out_specs = [pl.BlockSpec((c, RB, n), lambda i, pos: (0, i, 0))] * sides
    if want_zn:
        out_shape = out_shape + [jax.ShapeDtypeStruct((r, n, d), BF)]
        out_specs = out_specs + [pl.BlockSpec((RB, n, d), lambda i, pos: (i, 0, 0))]
    scratch = [pltpu.VMEM((RB, ka, n), BF), pltpu.VMEM((sides, RB, c, n), BF)]
    if len(zs) > 1:
        scratch = scratch + [pltpu.VMEM((RB, n, d), BF)]
    spec = pltpu.PrefetchScalarGridSpec(
        num_scalar_prefetch=1,
        grid=(r // RB,),
        in_specs=[pl.BlockSpec((RB, width, d), lambda i, pos: (i, 0, 0))] * len(zs)
        + [
            pl.BlockSpec((RB, n), lambda i, pos: (i, 0)),
            pl.BlockSpec((d, LANES), lambda i, pos: (0, 0)),
            pl.BlockSpec((d, LANES), lambda i, pos: (0, 0)),
            pl.BlockSpec(w.shape, lambda i, pos: (0, 0, 0, 0)),
        ],
        out_specs=out_specs,
        scratch_shapes=scratch,
    )
    return pl.pallas_call(
        functools.partial(proj_kernel, sides, len(zs), want_zn),
        grid_spec=spec,
        out_shape=out_shape,
        name="project",
        cost_estimate=pl.CostEstimate(flops=16 * sides * r * n * d * c, bytes_accessed=2 * r * n * d * (2 + sides), transcendentals=0),
        compiler_params=pltpu.CompilerParams(vmem_limit_bytes=40 << 20),
    )(pos, *zs, mask, scale, bias, w)


def tri_kernel(nb, cb, sc_ref, a_ref, b1_ref, b2_ref, z_ref, zn_ref, ls_ref, lb_ref, wo_ref, bo_ref, wg_ref, bg_ref, o_ref, acc, on):
    step = pl.program_id(0)
    c = acc.shape[0]
    j1 = b1_ref.shape[1]
    width = 2 * j1

    @pl.when(step < nb)
    def _():
        for k in range(cb):
            both = jnp.concatenate([b1_ref[k], b2_ref[k]], axis=0)
            acc[step * cb + k] = lax.dot_general(a_ref[k], both, (((1,), (1,)), ((), ())), preferred_element_type=F32)

    @pl.when(step >= nb)
    def _():
        ib = pl.multiple_of((step - nb) * RB, RB)
        zero = jnp.zeros((RB, width), F32)

        def block(k):
            return acc[pl.ds(pl.multiple_of(k * RB, RB), RB), pl.ds(ib, RB), :]

        mean = lax.fori_loop(0, c // RB, lambda k, t: t + jnp.sum(block(k), axis=0), zero) * (1.0 / c)

        def squares(k, t):
            v = block(k) - mean[None]
            return t + jnp.sum(v * v, axis=0)

        rstd = lax.rsqrt(lax.fori_loop(0, c // RB, squares, zero) * (1.0 / c) + LN_EPS)

        @pl.loop(0, c // RB)
        def _(k):
            k0 = pl.multiple_of(k * RB, RB)
            v = (block(k) - mean[None]) * rstd[None] * ls_ref[pl.ds(k0, RB), :, :width] + lb_ref[pl.ds(k0, RB), :, :width]
            on[:, pl.ds(k0, RB), :] = jnp.transpose(v.astype(BF), (1, 0, 2))

        off = pl.multiple_of(sc_ref[0], RB)
        offs = [off, pl.multiple_of(j1 - off, RB)]
        unroll = 4

        @pl.loop(0, RB, step=unroll)
        def _(i0):
            for t in range(unroll):
                i = i0 + t
                u = lax.dot_general(on[i], wo_ref[...], (((0,), (0,)), ((), ())), preferred_element_type=F32)
                u = (u + bo_ref[...]).astype(BF).astype(F32)
                for h in range(2):
                    at = pl.ds(offs[h], j1)
                    g = jnp.dot(zn_ref[i, at, :], wg_ref[...], preferred_element_type=F32) + bg_ref[...]
                    o_ref[i, at, :] = (z_ref[i, at, :].astype(F32) + jax.nn.sigmoid(g) * u[h * j1:(h + 1) * j1]).astype(BF)


def triangle(sc, a, b1, b2, z, zn, ls, lb, wo, bo, wg, bg):
    c, r, n = a.shape
    j1 = b1.shape[1]
    d = z.shape[2]
    cb = RB
    nb = c // cb

    def first(s, sc):
        return jnp.minimum(s, nb - 1), 0, 0

    def later(s):
        return jnp.maximum(s - nb, 0)

    def whole2(s, sc):
        return 0, 0

    def whole3(s, sc):
        return 0, 0, 0

    spec = pltpu.PrefetchScalarGridSpec(
        num_scalar_prefetch=1,
        grid=(nb + r // RB,),
        in_specs=[
            pl.BlockSpec((cb, r, n), first),
            pl.BlockSpec((cb, j1, n), first),
            pl.BlockSpec((cb, j1, n), first),
            pl.BlockSpec((RB, 2 * j1, d), lambda s, sc: (later(s), sc[2], 0)),
            pl.BlockSpec((RB, 2 * j1, d), lambda s, sc: (later(s), sc[1], 0)),
            pl.BlockSpec(ls.shape, whole3),
            pl.BlockSpec(lb.shape, whole3),
            pl.BlockSpec(wo.shape, whole2),
            pl.BlockSpec(bo.shape, whole2),
            pl.BlockSpec(wg.shape, whole2),
            pl.BlockSpec(bg.shape, whole2),
        ],
        out_specs=pl.BlockSpec((RB, 2 * j1, d), lambda s, sc: (later(s), 0, 0)),
        scratch_shapes=[pltpu.VMEM((c, r, 2 * j1), F32), pltpu.VMEM((RB, c, 2 * j1), BF)],
    )
    return pl.pallas_call(
        functools.partial(tri_kernel, nb, cb),
        grid_spec=spec,
        out_shape=jax.ShapeDtypeStruct((r, 2 * j1, d), BF),
        name="triangle",
        cost_estimate=pl.CostEstimate(flops=32 * r * n * j1 * c, bytes_accessed=2 * c * n * (r + 2 * j1), transcendentals=0),
        compiler_params=pltpu.CompilerParams(vmem_limit_bytes=40 << 20),
    )(sc, a, b1, b2, z, zn, ls, lb, wo, bo, wg, bg)


def pair_weight(w_pair, b_pair):
    d, c2 = w_pair.shape
    wide = jnp.concatenate([w_pair.T, b_pair[:, None], jnp.zeros((c2, 15), w_pair.dtype)], axis=1)
    value, gate = wide.reshape(2, 2, c2 // 4, d + 16)
    return jnp.concatenate([value, gate], axis=1)


def solution(mesh):
    row_spec = P(('batch', 'dap'), None, None)
    mask_spec = P(('batch', 'dap'), None)
    vec_spec = P(None, None)
    mat_spec = P(None, None, None)
    size = mesh.shape['dap']
    chips = size // 2
    side = [1 - 2 * (i % 2) for i in range(size)]
    to_helper = [(i, (i + 2 * side[i]) % size) for i in range(size)]
    to_other = [(i, (i - 2 * side[i]) % size) for i in range(size)]
    to_partner = [(i, i ^ 1) for i in range(size)]

    def send(x, perm):
        return lax.ppermute(x, 'dap', perm)

    def device_fn(z_rows, mask_rows, ln_in_scale, ln_in_bias, w_in, b_in, w_gate, b_gate, ln_out_scale, ln_out_bias, w_out, b_out):
        layers, d, hidden4 = w_in.shape
        rows = z_rows.shape[0]
        index = lax.axis_index('dap')
        core, chip = index % 2, index // 2
        sgn = 1 - 2 * core

        def place(k):
            return lax.rem(chip + k * sgn + 2 * chips, chips)

        zero = jnp.zeros((), jnp.int32)
        off = core * rows

        def scalars(block, zblock):
            return jnp.stack([off, block, zblock]).astype(jnp.int32)

        mask = mask_rows.astype(F32)
        z_near, z_other = send(z_rows, to_helper), send(z_rows, to_other)
        mask_near, mask_other = send(mask, to_helper), send(mask, to_other)
        z_own, near, other = [z_rows], [z_near], [z_other]

        for layer in range(layers):
            h2 = hidden4 // 2
            w = jnp.stack([pair_weight(w_in[layer, :, :h2], b_in[layer, :h2]), pair_weight(w_in[layer, :, h2:], b_in[layer, h2:])])
            scale = jnp.broadcast_to(ln_in_scale[layer].astype(F32)[:, None], (d, LANES))
            bias = jnp.broadcast_to(ln_in_bias[layer].astype(F32)[:, None], (d, LANES))
            ls = jnp.broadcast_to(ln_out_scale[layer].astype(F32)[:, None, None], (h2 // 2, 1, LANES))
            lb = jnp.broadcast_to(ln_out_bias[layer].astype(F32)[:, None, None], (h2 // 2, 1, LANES))
            tail = (ls, lb, w_out[layer], b_out[layer].astype(F32)[None], w_gate[layer], b_gate[layer].astype(F32)[None])
            first = layer == 0
            pos_own = jnp.stack([place(0), place(1), place(-1), place(2)])
            pos_near = jnp.stack([place(-1), place(0), place(-2), place(1)])
            pos_other = jnp.stack([place(1), place(2), place(0), place(-1)])

            a_own, b_own, zn_own = project(z_own, pos_own, mask, scale, bias, w, True)
            b_own_p = send(b_own, to_partner)
            z0 = z_own[0]
            p0 = triangle(scalars(place(0), place(0) if first else zero), a_own, b_own, b_own_p, z0, zn_own, *tail)

            a_near, b_near, zn_near = project(near, pos_near, mask_near, scale, bias, w, True)
            b_near_p = send(b_near, to_partner)
            b_other, = project(other, pos_other, mask_other, scale, bias, w[1:], False)
            b_other_p = send(b_other, to_partner)
            zf = near[0] if first else near[3]
            far = triangle(scalars(place(1), place(1) if first else zero), a_near, b_other, b_near_p, zf, zn_near, *tail)
            p3 = send(far, to_other)
            z1 = z_own[0] if first else z_own[1]
            z2 = z_own[0] if first else z_own[2]
            p1 = triangle(scalars(place(1), place(1) if first else zero), a_own, b_other, b_near_p, z1, zn_own, *tail)
            p2 = triangle(scalars(place(-1), place(-1) if first else zero), a_own, b_near, b_other_p, z2, zn_own, *tail)
            own = [p0, p1, p2, p3]
            if layer + 1 < layers:
                near = [send(p, to_helper) for p in own[:3]] + [far]
                other = [send(p, to_other) for p in own]
            z_own = own

        out = jnp.zeros_like(z_rows)
        width = z_own[0].shape[1]
        for q, piece in zip([place(0), place(1), place(-1), place(2)], z_own):
            out = lax.dynamic_update_slice(out, piece, (zero, q * width, zero))
        return out

    return jax.shard_map(device_fn, mesh=mesh, in_specs=(row_spec, mask_spec, vec_spec, vec_spec, mat_spec, vec_spec, mat_spec, vec_spec, vec_spec, vec_spec, mat_spec, vec_spec), out_specs=row_spec, check_vma=False)
```

```python
import functools

import jax
import jax.numpy as jnp
from jax import lax
from jax.experimental import pallas as pl
from jax.experimental.pallas import tpu as pltpu
from jax.sharding import PartitionSpec as P


LN_EPS = 1e-5
F32 = jnp.float32
BF = jnp.bfloat16
RB = 16
LANES = 128
VMEM = 67043328
ROWS_AT_ONCE = 8
ANY = pl.BlockSpec(memory_space=pl.ANY)


def norm_columns(x, scale, bias):
    inv = 1.0 / x.shape[0]
    cen = x - jnp.sum(x, axis=0, keepdims=True) * inv
    var = jnp.sum(cen * cen, axis=0, keepdims=True) * inv
    return (cen * lax.rsqrt(var + LN_EPS) * scale + bias).astype(BF)


def fill(dst, piece_refs, pos_ref, segments):
    at = 0
    for ref, lengths in zip(piece_refs, segments):
        start = 0
        for length in lengths:
            dst[:, pl.ds(pl.multiple_of(pos_ref[at], RB), length), :] = ref[:, start:start + length, :]
            start += length
            at += 1


def proj_kernel(sides, segments, keep, extra, pos_ref, *refs):
    pieces = len(segments)
    z_refs, refs = refs[:pieces], refs[pieces:]
    m_ref, s_ref, b_ref, w_ref = refs[:4]
    refs = refs[4 + extra:]
    outs, refs = refs[:sides], refs[sides:]
    if keep:
        (zn_ref, zfull), refs = refs[:2], refs[2:]
    else:
        zfull, refs = refs[-1], refs[:-1]
    znm, tmp = refs
    rows, n, d = zfull.shape
    ka = znm.shape[1]
    fill(zfull, z_refs, pos_ref, segments)
    ones_row = lax.broadcasted_iota(jnp.int32, (ka - d, LANES), 0) == 0
    unroll = 4

    @pl.loop(0, rows, step=unroll)
    def _(i0):
        for u in range(unroll):
            i = i0 + u
            m = m_ref[pl.ds(i, 1), :]
            for t in range(n // LANES):
                sl = slice(t * LANES, (t + 1) * LANES)
                y = norm_columns(zfull[i, sl, :].T.astype(F32), s_ref[...], b_ref[...])
                if keep:
                    zn_ref[i, sl, :] = y.T
                znm[i, :d, sl] = y * m[:, sl].astype(BF)
                znm[i, d:, sl] = jnp.where(ones_row, jnp.broadcast_to(m[:, sl], ones_row.shape), 0.0).astype(BF)

    parts, half = w_ref.shape[1], w_ref.shape[2] // 2

    @pl.loop(0, rows, unroll=ROWS_AT_ONCE)
    def _(i):
        rhs = znm[i]
        for sd in range(sides):
            for h in range(parts):
                p = jnp.dot(w_ref[sd, h], rhs, preferred_element_type=F32)
                tmp[sd, i, h * half:(h + 1) * half, :] = (jax.nn.sigmoid(p[half:]) * p[:half]).astype(BF)

    @pl.loop(0, parts * half // RB, unroll=2)
    def _(k):
        k0 = pl.multiple_of(k * RB, RB)
        for sd in range(sides):
            outs[sd][pl.ds(k0, RB)] = jnp.transpose(tmp[sd, :, pl.ds(k0, RB), :], (1, 0, 2))


def project(pieces, pos, mask, scale, bias, w, r0, r, total, keep=None, deps=()):
    n = mask.shape[1]
    d = pieces[0][0].shape[2]
    sides, parts, half2, ka = w.shape
    c = parts * half2 // 2
    blk = r0 // RB
    full = sides == 2
    b_shape, b_spec = jax.ShapeDtypeStruct((c, r, n), BF), pl.BlockSpec((c, RB, n), lambda i, pos: (0, i, 0))
    out_shape, out_specs = [b_shape], [b_spec]
    if full:
        out_shape = [jax.ShapeDtypeStruct((c, total, n), BF), b_shape] + [jax.ShapeDtypeStruct((total, n, d), BF)] * 2
        out_specs = [pl.BlockSpec((c, RB, n), lambda i, pos: (0, i + blk, 0)), b_spec] + [pl.BlockSpec((RB, n, d), lambda i, pos: (i + blk, 0, 0))] * 2
    scratch = [pltpu.VMEM((RB, ka, n), BF), pltpu.VMEM((sides, RB, c, n), BF)]
    if not full:
        scratch = scratch + [pltpu.VMEM((RB, n, d), BF)]
    keep = tuple(keep or ())
    extra = keep + tuple(deps)
    count = len(pieces)
    spec = pltpu.PrefetchScalarGridSpec(
        num_scalar_prefetch=1,
        grid=(r // RB,),
        in_specs=[pl.BlockSpec((RB, x.shape[1], d), functools.partial(lambda f, i, pos: (i + f, 0, 0), f // RB)) for x, f, _ in pieces]
        + [
            pl.BlockSpec((RB, n), lambda i, pos: (i + blk, 0)),
            pl.BlockSpec((d, LANES), lambda i, pos: (0, 0)),
            pl.BlockSpec((d, LANES), lambda i, pos: (0, 0)),
            pl.BlockSpec(w.shape, lambda i, pos: (0, 0, 0, 0)),
        ]
        + [ANY] * len(extra),
        out_specs=out_specs,
        scratch_shapes=scratch,
    )
    first = 1 + count + 4
    return pl.pallas_call(
        functools.partial(proj_kernel, sides, [g for _, _, g in pieces], full, len(extra)),
        grid_spec=spec,
        out_shape=out_shape,
        name="project",
        input_output_aliases={first: 0, first + 1: 2, first + 2: 3} if keep else {},
        cost_estimate=pl.CostEstimate(flops=16 * sides * r * n * d * c, bytes_accessed=2 * r * n * d * (2 + sides), transcendentals=0),
        compiler_params=pltpu.CompilerParams(vmem_limit_bytes=VMEM),
    )(pos, *[x for x, _, _ in pieces], mask, scale, bias, w, *extra)


def tri_kernel(nb, cb, widths, split, extra, pos_ref, a_ref, *refs):
    b_refs, refs = refs[:len(widths)], refs[len(widths):]
    z_ref, zn_ref, ls_ref, lb_ref, wo_ref, bo_ref, wg_ref, bg_ref = refs[:8]
    refs = refs[8 + extra:]
    outs, (acc, on, res) = refs[:-3], refs[-3:]
    step = pl.program_id(0)
    c = acc.shape[0]
    width = sum(widths)

    @pl.when(step < nb)
    def _():
        for k in range(cb):
            both = jnp.concatenate([b[k] for b in b_refs], axis=0)
            acc[step * cb + k] = lax.dot_general(a_ref[k], both, (((1,), (1,)), ((), ())), preferred_element_type=F32)

    @pl.when(step >= nb)
    def _():
        ib = pl.multiple_of((step - nb) * RB, RB)
        zero = jnp.zeros((RB, width), F32)

        def block(k):
            return acc[pl.ds(pl.multiple_of(k * RB, RB), RB), pl.ds(ib, RB), :]

        mean = lax.fori_loop(0, c // RB, lambda k, t: t + jnp.sum(block(k), axis=0), zero) * (1.0 / c)

        def squares(k, t):
            v = block(k) - mean[None]
            return t + jnp.sum(v * v, axis=0)

        rstd = lax.rsqrt(lax.fori_loop(0, c // RB, squares, zero) * (1.0 / c) + LN_EPS)

        @pl.loop(0, c // RB)
        def _(k):
            k0 = pl.multiple_of(k * RB, RB)
            v = (block(k) - mean[None]) * rstd[None] * ls_ref[pl.ds(k0, RB), :, :width] + lb_ref[pl.ds(k0, RB), :, :width]
            on[:, pl.ds(k0, RB), :] = jnp.transpose(v.astype(BF), (1, 0, 2))

        g_rows = ROWS_AT_ONCE

        @pl.loop(0, RB, step=g_rows)
        def _(i0):
            rs = pl.ds(i0, g_rows)
            ont = jnp.transpose(on[rs], (0, 2, 1)).reshape(g_rows * width, c)
            u = jnp.dot(ont, wo_ref[...], preferred_element_type=F32) + bo_ref[...]
            u = u.astype(BF).astype(F32).reshape(g_rows, width, -1)
            start = 0
            for h, wd in enumerate(widths):
                at = pl.ds(pl.multiple_of(pos_ref[h], RB), wd)
                g = jnp.dot(zn_ref[rs, at, :].reshape(g_rows * wd, -1), wg_ref[...], preferred_element_type=F32) + bg_ref[...]
                gu = jax.nn.sigmoid(g).reshape(g_rows, wd, -1) * u[:, start:start + wd]
                res[rs, start:start + wd, :] = (z_ref[rs, at, :].astype(F32) + gu).astype(BF)
                start += wd

        if split is None:
            outs[0][...] = res[...]
        else:
            @pl.when(step - nb < split)
            def _():
                outs[0][...] = res[...]

            @pl.when(step - nb >= split)
            def _():
                outs[1][...] = res[...]


def triangle(pos, a, bs, z, zn, tail, split=None, deps=()):
    c, r, n = a.shape
    d = z.shape[2]
    cb = RB
    nb = c // cb
    widths = [b.shape[1] for b in bs]
    width = sum(widths)

    def first(s, pos):
        return jnp.minimum(s, nb - 1), 0, 0

    def later(s):
        return jnp.maximum(s - nb, 0)

    def whole2(s, pos):
        return 0, 0

    def whole3(s, pos):
        return 0, 0, 0

    def rows_of(s, pos):
        return later(s), 0, 0

    if split is None:
        out_shape = [jax.ShapeDtypeStruct((r, width, d), BF)]
        out_specs = [pl.BlockSpec((RB, width, d), rows_of)]
        cut = None
    else:
        cut = split // RB
        out_shape = [jax.ShapeDtypeStruct((k, width, d), BF) for k in (split, r - split)]
        out_specs = [
            pl.BlockSpec((RB, width, d), lambda s, pos: (jnp.minimum(later(s), cut - 1), 0, 0)),
            pl.BlockSpec((RB, width, d), lambda s, pos: (jnp.maximum(later(s) - cut, 0), 0, 0)),
        ]
    spec = pltpu.PrefetchScalarGridSpec(
        num_scalar_prefetch=1,
        grid=(nb + r // RB,),
        in_specs=[pl.BlockSpec((cb, r, n), first)]
        + [pl.BlockSpec((cb, j, n), first) for j in widths]
        + [pl.BlockSpec((RB, n, d), rows_of), pl.BlockSpec((RB, n, d), rows_of)]
        + [pl.BlockSpec(x.shape, whole3 if x.ndim == 3 else whole2) for x in tail]
        + [ANY] * len(deps),
        out_specs=out_specs,
        scratch_shapes=[pltpu.VMEM((c, r, width), F32), pltpu.VMEM((RB, c, width), BF), pltpu.VMEM((RB, width, d), BF)],
    )
    return pl.pallas_call(
        functools.partial(tri_kernel, nb, cb, widths, cut, len(deps)),
        grid_spec=spec,
        out_shape=out_shape,
        name="triangle",
        cost_estimate=pl.CostEstimate(flops=16 * r * n * width * c, bytes_accessed=2 * c * n * (r + width), transcendentals=0),
        compiler_params=pltpu.CompilerParams(vmem_limit_bytes=VMEM),
    )(pos, a, *bs, z, zn, *tail, *deps)


def assemble_kernel(segments, pos_ref, *refs):
    fill(refs[-1], refs[:-1], pos_ref, segments)


def assemble(pieces, pos, n):
    r, _, d = pieces[0][0].shape
    spec = pltpu.PrefetchScalarGridSpec(
        num_scalar_prefetch=1,
        grid=(r // RB,),
        in_specs=[pl.BlockSpec((RB, x.shape[1], d), lambda i, pos: (i, 0, 0)) for x, _ in pieces],
        out_specs=pl.BlockSpec((RB, n, d), lambda i, pos: (i, 0, 0)),
    )
    return pl.pallas_call(
        functools.partial(assemble_kernel, [g for _, g in pieces]),
        grid_spec=spec,
        out_shape=jax.ShapeDtypeStruct((r, n, d), BF),
        name="assemble",
    )(pos, *[x for x, _ in pieces])


def pair_weight(w_pair, b_pair):
    d, c2 = w_pair.shape
    wide = jnp.concatenate([w_pair.T, b_pair[:, None], jnp.zeros((c2, 15), w_pair.dtype)], axis=1)
    value, gate = wide.reshape(2, 2, c2 // 4, d + 16)
    return jnp.concatenate([value, gate], axis=1)


def solution(mesh):
    row_spec = P(('batch', 'dap'), None, None)
    mask_spec = P(('batch', 'dap'), None)
    vec_spec = P(None, None)
    mat_spec = P(None, None, None)
    size = mesh.shape['dap']
    chips = size // 2
    side = [1 - 2 * (i % 2) for i in range(size)]
    to_helper = [(i, (i + 2 * side[i]) % size) for i in range(size)]
    to_other = [(i, (i - 2 * side[i]) % size) for i in range(size)]
    to_partner = [(i, i ^ 1) for i in range(size)]

    def device_fn(z_rows, mask_rows, ln_in_scale, ln_in_bias, w_in, b_in, w_gate, b_gate, ln_out_scale, ln_out_bias, w_out, b_out):
        def send(x, perm):
            return lax.ppermute(x, 'dap', perm)

        layers, d, hidden4 = w_in.shape
        h2 = hidden4 // 2
        rows, n, _ = z_rows.shape
        lo = RB
        hi = rows - lo
        parts = ((0, hi), (hi, lo))
        index = lax.axis_index('dap')
        core, chip = index % 2, index // 2
        sgn = 1 - 2 * core

        def columns(segs, shift=0):
            at = [2 * rows * lax.rem(chip + (k + shift) * sgn + 4 * chips, chips) + rows * jnp.where(flip, 1 - core, core) + r0 for k, flip, r0, _ in segs]
            return jnp.stack(at).astype(jnp.int32)

        def lengths(segs):
            return [g[3] for g in segs]

        def both_cores(k):
            return [(k, flip, r0, r) for r0, r in parts for flip in (0, 1)]

        mid = [[(k, flip, r0, r) for k in (1, -1) for flip in (0, 1)] for r0, r in parts]
        kinds = [both_cores(0), mid[0], mid[1], both_cores(2)]
        every = [g for kind in kinds for g in kind]

        z_hi, z_lo = z_rows[:hi], z_rows[hi:]
        near_in, other_in = [None, None], [None, None]
        near_in[0], other_in[0] = send(z_hi, to_helper), send(z_hi, to_other)
        mask = mask_rows.astype(F32)
        mask_near, mask_other = send(mask, to_helper), send(mask, to_other)
        near_in[1], other_in[1] = send(z_lo, to_helper), send(z_lo, to_other)

        start = jnp.zeros((1,), jnp.int32)
        own_p = [[(z_rows, r0, [n])] for r0, _ in parts]
        near_p = [[(x, 0, [n])] for x in near_in]
        other_p = [[(x, 0, [n])] for x in other_in]
        pos = [start] * 3
        last = ()

        for layer in range(layers):
            w = jnp.stack([pair_weight(w_in[layer, :, :h2], b_in[layer, :h2]), pair_weight(w_in[layer, :, h2:], b_in[layer, h2:])])
            scale = jnp.broadcast_to(ln_in_scale[layer].astype(F32)[:, None], (d, LANES))
            bias = jnp.broadcast_to(ln_in_bias[layer].astype(F32)[:, None], (d, LANES))
            ls = jnp.broadcast_to(ln_out_scale[layer].astype(F32)[:, None, None], (h2 // 2, 1, LANES))
            lb = jnp.broadcast_to(ln_out_bias[layer].astype(F32)[:, None, None], (h2 // 2, 1, LANES))
            tail = (ls, lb, w_out[layer], b_out[layer].astype(F32)[None], w_gate[layer], b_gate[layer].astype(F32)[None])
            final = layer + 1 == layers

            def side_of(pieces, where, m, part, sides, keep, deps):
                r0, r = parts[part]
                return project(pieces, where, m, scale, bias, w[2 - sides:], r0, r, rows, keep, deps)

            b = [None, None]
            b_p = [None, None]
            bn, bn_p, bo, bo_p = [None] * 2, [None] * 2, [None] * 2, [None] * 2
            own = near = None
            for part in (0, 1):
                a_, b[part], zn_, z_ = side_of(own_p[part], pos[0], mask, part, 2, own, last)
                own = (a_, zn_, z_)
                last = (b[part],)
                b_p[part] = send(b[part], to_partner)
                if layer > 0 and part == 0:
                    other_p[1] = other_pieces(1)
            if layer == 0:
                p0, = triangle(columns(kinds[0]), own[0], [b[0], b_p[0], b[1], b_p[1]], own[2], own[1], tail, None, last)
                last = (p0,)
                p0_near, p0_other = send(p0, to_helper), send(p0, to_other)
            for part in (0, 1):
                a_, bn[part], zn_, z_ = side_of(near_p[part], pos[1], mask_near, part, 2, near, last)
                near = (a_, zn_, z_)
                last = (bn[part],)
                bn_p[part] = send(bn[part], to_partner)
                bo[part], = side_of(other_p[part], pos[2], mask_other, part, 1, None, last)
                last = (bo[part],)
                bo_p[part] = send(bo[part], to_partner)
                if part == 0:
                    if layer > 0:
                        p0, = triangle(columns(kinds[0]), own[0], [b[0], b_p[0], b[1], b_p[1]], own[2], own[1], tail, None, last)
                        last = (p0,)
                    c1 = triangle(columns(kinds[1]), own[0], [bo[0], bn_p[0], bn[0], bo_p[0]], own[2], own[1], tail, None if final else hi, last)
                    last = (c1[0],)
                    if not final:
                        c1_near, c1_other = [send(c1[0], to_helper)], [send(c1[0], to_other)]
            far = triangle(columns(kinds[3], -1), near[0], [bo[0], bn_p[0], bo[1], bn_p[1]], near[2], near[1], tail, None if final else hi, last)
            last = (far[0],)
            p3 = [send(x, to_other) for x in far]
            c2 = triangle(columns(kinds[2]), own[0], [bo[1], bn_p[1], bn[1], bo_p[1]], own[2], own[1], tail, None if final else hi, last)
            last = (c2[0],)
            if final:
                return assemble([(x, lengths(g)) for x, g in zip((p0, c1[0], c2[0], p3[0]), kinds)], columns(every), n)

            c2_near, c2_other = [send(c2[0], to_helper)], [send(c2[0], to_other)]
            for got, x in ((c1_near, c1), (c2_near, c2)):
                got.append(send(x[1], to_helper))
            for got, x in ((c1_other, c1), (c2_other, c2)):
                got.append(send(x[1], to_other))

            def group(x0, x1, x2, x3, part):
                return [(x, parts[part][0] if q == 0 else 0, lengths(kinds[q])) for q, x in enumerate((x0, x1, x2, x3))]

            own_p = [group(p0, c1[k], c2[k], p3[k], k) for k in (0, 1)]
            near_p = [group(p0_near, c1_near[k], c2_near[k], far[k], k) for k in (0, 1)]

            def other_pieces(k):
                return group(p0_other, c1_other[k], c2_other[k], send(p3[k], to_other), k)

            other_p = [other_pieces(0), None]
            pos = [columns(every), columns(every, -1), columns(every, 1)]

    return jax.shard_map(device_fn, mesh=mesh, in_specs=(row_spec, mask_spec, vec_spec, vec_spec, mat_spec, vec_spec, mat_spec, vec_spec, vec_spec, vec_spec, mat_spec, vec_spec), out_specs=row_spec, check_vma=False)
```

```python
import functools

import jax
import jax.numpy as jnp
from jax import lax
from jax.experimental import pallas as pl
from jax.experimental.pallas import tpu as pltpu
from jax.sharding import PartitionSpec as P


LN_EPS = 1e-5
F32 = jnp.float32
BF = jnp.bfloat16
RB = 16
LANES = 128
VMEM = 67043328
ROWS_AT_ONCE = 8
PAIRS = 4
ANY = pl.BlockSpec(memory_space=pl.ANY)


def norm_columns(x, scale, bias):
    inv = 1.0 / x.shape[0]
    cen = x - jnp.sum(x, axis=0, keepdims=True) * inv
    var = jnp.sum(cen * cen, axis=0, keepdims=True) * inv
    return (cen * lax.rsqrt(var + LN_EPS) * scale + bias).astype(BF)


def fill(dst, piece_refs, pos_ref, segments):
    at = 0
    for ref, lengths in zip(piece_refs, segments):
        start = 0
        for length in lengths:
            dst[:, pl.ds(pl.multiple_of(pos_ref[at], RB), length), :] = ref[:, start:start + length, :]
            start += length
            at += 1
    return at


def proj_kernel(sides, segments, chosen, z_out, extra, pos_ref, *refs):
    pieces = len(segments)
    z_refs, refs = refs[:pieces], refs[pieces:]
    m_ref, s_ref, b_ref, w_ref = refs[:4]
    refs = refs[4 + extra:]
    outs, refs = refs[:sides], refs[sides:]
    keep = sides == 2
    if keep:
        zn_out, refs = refs[0], refs[1:]
    if z_out:
        zkept, refs = refs[0], refs[1:]
    znm, tmp = refs[:2]
    refs = refs[2:]
    rows, n, d = z_refs[0].shape[0], m_ref.shape[1], z_refs[0].shape[2]
    ka = znm.shape[1]
    zfull = z_refs[0]
    at = len(segments[0])
    if pieces > 1:
        zfull, refs = (zkept, refs) if z_out and chosen is None else (refs[0], refs[1:])
        at = fill(zfull, z_refs, pos_ref, segments)
    zn_ref = None
    if keep:
        zn_ref = zn_out if chosen is None else refs[0]
    ones_row = lax.broadcasted_iota(jnp.int32, (ka - d, LANES), 0) == 0
    unroll = 4

    @pl.loop(0, rows, step=unroll)
    def _(i0):
        for u in range(unroll):
            i = i0 + u
            pair = i0 // 2 + u // 2
            m = m_ref[pl.ds(i, 1), :]
            for t in range(n // LANES):
                sl = slice(t * LANES, (t + 1) * LANES)
                wide = slice((u % 2) * n + t * LANES, (u % 2) * n + (t + 1) * LANES)
                y = norm_columns(zfull[i, sl, :].T.astype(F32), s_ref[...], b_ref[...])
                if keep:
                    zn_ref[i, sl, :] = y.T
                znm[pair, :d, wide] = y * m[:, sl].astype(BF)
                znm[pair, d:, wide] = jnp.where(ones_row, jnp.broadcast_to(m[:, sl], ones_row.shape), 0.0).astype(BF)

    parts, half = w_ref.shape[1], w_ref.shape[2] // 2

    @pl.loop(0, rows // 2, unroll=PAIRS)
    def _(i):
        rhs = znm[i]
        for sd in range(sides):
            for h in range(parts):
                p = jnp.dot(w_ref[sd, h], rhs, preferred_element_type=F32)
                act = ((jnp.tanh(p[half:]) + 1.0) * p[:half]).astype(BF)
                for e in range(2):
                    tmp[sd, 2 * i + e, h * half:(h + 1) * half, :] = act[:, e * n:(e + 1) * n]

    @pl.loop(0, parts * half // RB, unroll=2)
    def _(k):
        k0 = pl.multiple_of(k * RB, RB)
        for sd in range(sides):
            outs[sd][pl.ds(k0, RB)] = jnp.transpose(tmp[sd, :, pl.ds(k0, RB), :], (1, 0, 2))

    if chosen is not None:
        start = 0
        for length in chosen:
            place = pl.ds(pl.multiple_of(pos_ref[at], RB), length)
            zn_out[:, start:start + length, :] = zn_ref[:, place, :]
            zkept[:, start:start + length, :] = zfull[:, place, :]
            start += length
            at += 1


def project(pieces, pos, mask, params, layer, sides, r0, r, total, chosen=None, z_out=False, keep=None, deps=()):
    scale, bias, w = params
    n = mask.shape[1]
    d = pieces[0][0].shape[2]
    parts, half2, ka = w.shape[2:]
    c = parts * half2 // 2
    blk = r0 // RB
    full = sides == 2
    b_shape, b_spec = jax.ShapeDtypeStruct((c, r, n), BF), pl.BlockSpec((c, RB, n), lambda i, pos: (0, i, 0))
    out_shape, out_specs = [b_shape], [b_spec]
    width = n if chosen is None else sum(chosen)
    if full:
        kept = 2 if z_out else 1
        out_shape = [jax.ShapeDtypeStruct((c, total, n), BF), b_shape] + [jax.ShapeDtypeStruct((total, width, d), BF)] * kept
        out_specs = [pl.BlockSpec((c, RB, n), lambda i, pos: (0, i + blk, 0)), b_spec] + [pl.BlockSpec((RB, width, d), lambda i, pos: (i + blk, 0, 0))] * kept
    scratch = [pltpu.VMEM((RB // 2, ka, 2 * n), BF), pltpu.VMEM((sides, RB, c, n), BF)]
    count = len(pieces)
    if count > 1 and not (z_out and chosen is None):
        scratch = scratch + [pltpu.VMEM((RB, n, d), BF)]
    if chosen is not None:
        scratch = scratch + [pltpu.VMEM((RB, n, d), BF)]
    keep = tuple(keep or ())
    extra = keep + tuple(deps)
    spec = pltpu.PrefetchScalarGridSpec(
        num_scalar_prefetch=1,
        grid=(r // RB,),
        in_specs=[pl.BlockSpec((RB, x.shape[1], d), functools.partial(lambda f, i, pos: (i + f, 0, 0), f // RB)) for x, f, _ in pieces]
        + [
            pl.BlockSpec((RB, n), lambda i, pos: (i + blk, 0)),
            pl.BlockSpec((None, d, LANES), lambda i, pos: (layer, 0, 0)),
            pl.BlockSpec((None, d, LANES), lambda i, pos: (layer, 0, 0)),
            pl.BlockSpec((None, sides) + w.shape[2:], lambda i, pos: (layer, 2 - sides, 0, 0, 0)),
        ]
        + [ANY] * len(extra),
        out_specs=out_specs,
        scratch_shapes=scratch,
    )
    first = 1 + count + 4
    return pl.pallas_call(
        functools.partial(proj_kernel, sides, [g for _, _, g in pieces], chosen, z_out, len(extra)),
        grid_spec=spec,
        out_shape=out_shape,
        name="project",
        input_output_aliases={first: 0, first + 1: 2, first + 2: 3} if keep else {},
        cost_estimate=pl.CostEstimate(flops=16 * sides * r * n * d * c, bytes_accessed=2 * r * n * d * (2 + sides), transcendentals=0),
        compiler_params=pltpu.CompilerParams(vmem_limit_bytes=VMEM),
    )(pos, *[x for x, _, _ in pieces], mask, scale, bias, w, *extra)


def tri_kernel(nb, cb, widths, spread, extra, pos_ref, a_ref, *refs):
    count = len(widths)
    b_refs, z_refs, zn_refs, refs = refs[:count], refs[count:2 * count], refs[2 * count:3 * count], refs[3 * count:]
    ls_ref, lb_ref, wo_ref, bo_ref, wg_ref, bg_ref = refs[:6]
    o_ref, acc, on = refs[6 + extra:]
    step = pl.program_id(0)
    c = acc.shape[0]
    width = sum(widths)

    @pl.when(step < nb)
    def _():
        @pl.loop(0, cb, step=RB)
        def _(k0):
            for k in range(RB):
                both = jnp.concatenate([b[k0 + k] for b in b_refs], axis=0)
                acc[step * cb + k0 + k] = lax.dot_general(a_ref[k0 + k], both, (((1,), (1,)), ((), ())), preferred_element_type=F32)

    @pl.when(step >= nb)
    def _():
        ib = pl.multiple_of((step - nb) * RB, RB)
        zero = jnp.zeros((RB, width), F32)

        def block(k):
            return acc[pl.ds(pl.multiple_of(k * RB, RB), RB), pl.ds(ib, RB), :]

        mean = lax.fori_loop(0, c // RB, lambda k, t: t + jnp.sum(block(k), axis=0), zero) * (1.0 / c)

        def squares(k, t):
            v = block(k) - mean[None]
            return t + jnp.sum(v * v, axis=0)

        rstd = lax.rsqrt(lax.fori_loop(0, c // RB, squares, zero) * (1.0 / c) + LN_EPS)

        @pl.loop(0, c // RB)
        def _(k):
            k0 = pl.multiple_of(k * RB, RB)
            for t in range(0, width, LANES):
                sl = slice(t, min(t + LANES, width))
                v = acc[pl.ds(k0, RB), pl.ds(ib, RB), sl]
                lanes = sl.stop - sl.start
                v = (v - mean[None, :, sl]) * rstd[None, :, sl] * ls_ref[pl.ds(k0, RB), :, :lanes] + lb_ref[pl.ds(k0, RB), :, :lanes]
                on[:, pl.ds(k0, RB), sl] = jnp.transpose(v.astype(BF), (1, 0, 2))

        g_rows = ROWS_AT_ONCE

        @pl.loop(0, RB, step=g_rows)
        def _(i0):
            rs = pl.ds(i0, g_rows)
            start = 0
            for h, wd in enumerate(widths):
                ont = jnp.transpose(on[rs, :, start:start + wd], (0, 2, 1)).reshape(g_rows * wd, c)
                u = jnp.dot(ont, wo_ref[...], preferred_element_type=F32) + bo_ref[...]
                u = u.astype(BF).astype(F32)
                g = jnp.dot(zn_refs[h][rs].reshape(g_rows * wd, -1), wg_ref[...], preferred_element_type=F32) + bg_ref[...]
                new = z_refs[h][rs].astype(F32) + (jax.nn.sigmoid(g) * u).reshape(g_rows, wd, -1)
                at = pl.ds(pl.multiple_of(pos_ref[h], RB), wd) if spread else slice(start, start + wd)
                o_ref[rs, at, :] = new.astype(BF)
                start += wd


def triangle(pos, a, bs, z, zn, tail, layer, out_width=None, deps=()):
    c, r, n = a.shape
    d = z.shape[2]
    cb = 2 * RB
    nb = c // cb
    widths = [b.shape[1] for b in bs]
    width = sum(widths)

    def first(s, pos):
        return jnp.minimum(s, nb - 1), 0, 0

    def later(s):
        return jnp.maximum(s - nb, 0)

    def of_layer(x):
        return pl.BlockSpec((None,) + x.shape[1:], lambda s, pos: (layer,) + (0,) * (x.ndim - 1))

    def columns(h):
        return pl.BlockSpec((pl.Element(RB), pl.Element(widths[h]), pl.Element(d)), lambda s, pos: (later(s) * RB, pl.multiple_of(pos[h], RB), 0))

    wide = out_width or width
    spec = pltpu.PrefetchScalarGridSpec(
        num_scalar_prefetch=1,
        grid=(nb + r // RB,),
        in_specs=[pl.BlockSpec((cb, r, n), first)]
        + [pl.BlockSpec((cb, j, n), first) for j in widths]
        + [columns(h) for h in range(len(widths))] * 2
        + [of_layer(x) for x in tail]
        + [ANY] * len(deps),
        out_specs=pl.BlockSpec((RB, wide, d), lambda s, pos: (later(s), 0, 0)),
        scratch_shapes=[pltpu.VMEM((c, r, width), F32), pltpu.VMEM((RB, c, width), BF)],
    )
    return pl.pallas_call(
        functools.partial(tri_kernel, nb, cb, widths, out_width is not None, len(deps)),
        grid_spec=spec,
        out_shape=jax.ShapeDtypeStruct((r, wide, d), BF),
        name="triangle",
        cost_estimate=pl.CostEstimate(flops=16 * r * n * width * c, bytes_accessed=2 * c * n * (r + width), transcendentals=0),
        compiler_params=pltpu.CompilerParams(vmem_limit_bytes=VMEM),
    )(pos, a, *bs, *[z] * len(widths), *[zn] * len(widths), *tail, *deps)


def patch_kernel(pos_ref, piece_ref, whole_ref, out_ref):
    half = piece_ref.shape[1] // 2
    for h in range(2):
        out_ref[:, pl.ds(pl.multiple_of(pos_ref[1 + h], RB), half), :] = piece_ref[:, h * half:(h + 1) * half, :]


def patch(whole, piece, pos):
    r, j, d = piece.shape
    spec = pltpu.PrefetchScalarGridSpec(
        num_scalar_prefetch=1,
        grid=(r // RB,),
        in_specs=[pl.BlockSpec((RB, j, d), lambda i, pos: (i, 0, 0)), ANY],
        out_specs=pl.BlockSpec((RB, j, d), lambda i, pos: (i, pos[0], 0)),
    )
    return pl.pallas_call(
        patch_kernel,
        grid_spec=spec,
        out_shape=jax.ShapeDtypeStruct(whole.shape, BF),
        name="patch",
        input_output_aliases={2: 0},
    )(pos, piece, whole)


def side_weights(w_in, b_in):
    layers, d, c4 = w_in.shape
    w = jnp.transpose(w_in, (0, 2, 1))
    w = jnp.concatenate([w, b_in[:, :, None], jnp.zeros((layers, c4, 15), w_in.dtype)], axis=2) * 0.5
    w = w.reshape(layers, 2, 2, 2, c4 // 8, d + 16)
    return jnp.transpose(w, (0, 1, 3, 2, 4, 5)).reshape(layers, 2, 2, c4 // 4, d + 16)


def solution(mesh):
    row_spec = P(('batch', 'dap'), None, None)
    mask_spec = P(('batch', 'dap'), None)
    vec_spec = P(None, None)
    mat_spec = P(None, None, None)
    size = mesh.shape['dap']
    chips = size // 2
    side = [1 - 2 * (i % 2) for i in range(size)]
    to_helper = [(i, (i + 2 * side[i]) % size) for i in range(size)]
    to_other = [(i, (i - 2 * side[i]) % size) for i in range(size)]
    to_partner = [(i, i ^ 1) for i in range(size)]

    def device_fn(z_rows, mask_rows, ln_in_scale, ln_in_bias, w_in, b_in, w_gate, b_gate, ln_out_scale, ln_out_bias, w_out, b_out):
        def send(x, perm):
            return lax.ppermute(x, 'dap', perm)

        layers, d, _ = w_in.shape
        rows, n, _ = z_rows.shape
        lo = RB
        hi = rows - lo
        parts = ((0, hi), (hi, lo))
        index = lax.axis_index('dap')
        core, chip = index % 2, index // 2
        sgn = 1 - 2 * core

        def columns(segs, shift=0):
            at = [2 * rows * lax.rem(chip + (k + shift) * sgn + 4 * chips, chips) + rows * jnp.where(flip, 1 - core, core) + r0 for k, flip, r0, _ in segs]
            return jnp.stack(at).astype(jnp.int32)

        def lengths(segs):
            return [g[3] for g in segs]

        def whole(k):
            return [(k, flip, 0, rows) for flip in (0, 1)]

        mid = [[(k, flip, r0, r) for k in (1, -1) for flip in (0, 1)] for r0, r in parts]
        far_split = [(2, flip, r0, r) for r0, r in parts for flip in (0, 1)]

        z_hi = z_rows[:hi]
        near_in, other_in = [send(z_hi, to_helper)], [send(z_hi, to_other)]
        z_lo = z_rows[hi:]
        near_in.append(send(z_lo, to_helper))
        other_in.append(send(z_lo, to_other))
        mask = mask_rows.astype(F32)
        mask_near, mask_other = send(mask, to_helper), send(mask, to_other)

        scale = jnp.broadcast_to(ln_in_scale.astype(F32)[:, :, None], (layers, d, LANES))
        bias = jnp.broadcast_to(ln_in_bias.astype(F32)[:, :, None], (layers, d, LANES))
        params = (scale, bias, side_weights(w_in, b_in))
        c = ln_out_scale.shape[1]
        ls = jnp.broadcast_to(ln_out_scale.astype(F32)[:, :, None, None], (layers, c, 1, LANES))
        lb = jnp.broadcast_to(ln_out_bias.astype(F32)[:, :, None, None], (layers, c, 1, LANES))
        tail = (ls, lb, w_out, b_out.astype(F32)[:, None], w_gate, b_gate.astype(F32)[:, None])

        start = jnp.zeros((1,), jnp.int32)
        own_p, near_p, other_p, pos = None, None, None, None

        for layer in range(layers):
            final = layer + 1 == layers
            if layer == 0:
                far_segs = far_split
                a, b, zn = project([(z_rows, 0, [n])], start, mask, params, layer, 2, 0, rows, rows)
                b_p = send(b, to_partner)
                z_own = z_rows
                p0 = triangle(columns(whole(0)), a, [b, b_p], z_own, zn, tail, layer, None, (b,))
                p0_near, p0_other = send(p0, to_helper), send(p0, to_other)
                last = (p0,)
                near = None
                bn, bn_p, bo, bo_p = [None] * 2, [None] * 2, [None] * 2, [None] * 2
                for q, (r0, r) in enumerate(parts):
                    where = jnp.concatenate([start, columns(far_segs, -1)])
                    a_n, bn[q], zn_n, z_n = project([(near_in[q], 0, [n])], where, mask_near, params, layer, 2, r0, r, rows, lengths(far_segs), True, near, last)
                    near = (a_n, zn_n, z_n)
                    bn_p[q] = send(bn[q], to_partner)
                    bo[q], = project([(other_in[q], 0, [n])], start, mask_other, params, layer, 1, r0, r, rows, None, False, None, (bn[q],))
                    last = (bo[q],)
                    bo_p[q] = send(bo[q], to_partner)
                    if q == 0:
                        c1 = triangle(columns(mid[0]), a, [bo[0], bn_p[0], bn[0], bo_p[0]], z_own, zn, tail, layer, None, last)
                        last = (c1,)
                        c1_near, c1_other = send(c1, to_helper), send(c1, to_other)
                far_b = [bo[0], bn_p[0], bo[1], bn_p[1]]
            else:
                far_segs = whole(2)
                a, b, zn, z_own = project(own_p, pos[0], mask, params, layer, 2, 0, rows, rows, None, True, None, last)
                b_p = send(b, to_partner)
                where = jnp.concatenate([pos[1], columns(far_segs, -1)])
                a_n, bn, zn_n, z_n = project(near_p, where, mask_near, params, layer, 2, 0, rows, rows, lengths(far_segs), True, None, (b,))
                near = (a_n, zn_n, z_n)
                bn_p = send(bn, to_partner)
                bo, = project(other_p, pos[2], mask_other, params, layer, 1, 0, rows, rows, None, False, None, (bn,))
                bo_p = send(bo, to_partner)
                last = (bo,)
                far_b = [bo, bn_p]
            at, ends = 0, []
            for x in far_b:
                ends.append(at)
                at += x.shape[1]
            far = triangle(jnp.array(ends, jnp.int32), near[0], far_b, near[2], near[1], tail, layer, None, last)
            last = (far,)
            p3 = send(far, to_other)
            if layer == 0:
                c2 = triangle(columns(mid[1]), a, [bo[1], bn_p[1], bn[1], bo_p[1]], z_own, zn, tail, layer, None, last)
                last = (c2,)
                pieces = [(p0, whole(0)), (c1, mid[0]), (c2, mid[1])]
                near_got, other_got = [p0_near, c1_near, send(c2, to_helper)], [p0_other, c1_other, send(c2, to_other)]
            else:
                segs = whole(0) + whole(1) + whole(-1)
                rest = triangle(columns(segs), a, [b, b_p, bo, bn_p, bn, bo_p], z_own, zn, tail, layer, n if final else None, last)
                last = (rest,)
                if final:
                    block = lax.rem(chip + 2, chips)
                    return patch(rest, p3, jnp.stack([block, core * rows, (1 - core) * rows]).astype(jnp.int32))
                pieces = [(rest, segs)]
                near_got, other_got = [send(rest, to_helper)], [send(rest, to_other)]
            pieces.append((p3, far_segs))
            near_got.append(far)
            other_got.append(send(p3, to_other))
            every = [g for _, segs in pieces for g in segs]
            own_p = [(x, 0, lengths(segs)) for x, segs in pieces]
            near_p = [(x, 0, lengths(segs)) for x, (_, segs) in zip(near_got, pieces)]
            other_p = [(x, 0, lengths(segs)) for x, (_, segs) in zip(other_got, pieces)]
            pos = [columns(every), columns(every, -1), columns(every, 1)]

    return jax.shard_map(device_fn, mesh=mesh, in_specs=(row_spec, mask_spec, vec_spec, vec_spec, mat_spec, vec_spec, mat_spec, vec_spec, vec_spec, vec_spec, mat_spec, vec_spec), out_specs=row_spec, check_vma=False)
```

```python
import functools

import jax
import jax.numpy as jnp
from jax import lax
from jax.experimental import pallas as pl
from jax.experimental.pallas import tpu as pltpu
from jax.sharding import PartitionSpec as P


LN_EPS = 1e-5
F32 = jnp.float32
BF = jnp.bfloat16
RB = 16
LANES = 128
VMEM = 67043328
ROWS_AT_ONCE = 8
PAIRS = 4
CHANNELS = 16
ANY = pl.BlockSpec(memory_space=pl.ANY)


def norm_columns(x, scale, bias):
    inv = 1.0 / x.shape[0]
    cen = x - jnp.sum(x, axis=0, keepdims=True) * inv
    var = jnp.sum(cen * cen, axis=0, keepdims=True) * inv
    return (cen * lax.rsqrt(var + LN_EPS) * scale + bias).astype(BF)


def fill(dst, piece_refs, pos_ref, segments):
    at = 0
    for ref, lengths in zip(piece_refs, segments):
        start = 0
        for length in lengths:
            dst[:, pl.ds(pl.multiple_of(pos_ref[at], RB), length), :] = ref[:, start:start + length, :]
            start += length
            at += 1
    return at


def proj_kernel(sides, segments, chosen, z_out, extra, pos_ref, *refs):
    pieces = len(segments)
    z_refs, refs = refs[:pieces], refs[pieces:]
    m_ref, s_ref, b_ref, w_ref = refs[:4]
    refs = refs[4 + extra:]
    outs, refs = refs[:sides], refs[sides:]
    keep = sides == 2
    if keep:
        zn_out, refs = refs[0], refs[1:]
    if z_out:
        zkept, refs = refs[0], refs[1:]
    znm, tmp = refs[:2]
    refs = refs[2:]
    rows, n, d = z_refs[0].shape[0], m_ref.shape[1], z_refs[0].shape[2]
    ka = znm.shape[1]
    zfull = z_refs[0]
    at = len(segments[0])
    if pieces > 1:
        zfull, refs = (zkept, refs) if z_out and chosen is None else (refs[0], refs[1:])
        at = fill(zfull, z_refs, pos_ref, segments)
    zn_ref = None
    if keep:
        zn_ref = zn_out if chosen is None else refs[0]
    ones_row = lax.broadcasted_iota(jnp.int32, (ka - d, LANES), 0) == 0
    parts, half = w_ref.shape[1], w_ref.shape[2] // 2

    def norm_rows(pair):
        for u in range(2):
            i = 2 * pair + u
            m = m_ref[pl.ds(i, 1), :]
            for t in range(n // LANES):
                sl = slice(t * LANES, (t + 1) * LANES)
                wide = slice(u * n + t * LANES, u * n + (t + 1) * LANES)
                y = norm_columns(zfull[i, sl, :].T.astype(F32), s_ref[...], b_ref[...])
                if keep:
                    zn_ref[i, sl, :] = y.T
                znm[pair, :d, wide] = y * m[:, sl].astype(BF)
                znm[pair, d:, wide] = jnp.where(ones_row, jnp.broadcast_to(m[:, sl], ones_row.shape), 0.0).astype(BF)

    def sides_of(pair):
        rhs = znm[pair]
        for sd in range(sides):
            for h in range(parts):
                p = jnp.dot(w_ref[sd, h], rhs, preferred_element_type=F32)
                act = ((jnp.tanh(p[half:]) + 1.0) * p[:half]).astype(BF)
                for e in range(2):
                    tmp[sd, 2 * pair + e, h * half:(h + 1) * half, :] = act[:, e * n:(e + 1) * n]

    group = PAIRS
    for q in range(group):
        norm_rows(q)

    @pl.loop(0, rows // 2 - group, step=group)
    def _(pair):
        for q in range(group):
            sides_of(pair + q)
            norm_rows(pair + group + q)

    for q in range(group):
        sides_of(rows // 2 - group + q)

    @pl.loop(0, parts * half // RB, unroll=2)
    def _(k):
        k0 = pl.multiple_of(k * RB, RB)
        for sd in range(sides):
            outs[sd][pl.ds(k0, RB)] = jnp.transpose(tmp[sd, :, pl.ds(k0, RB), :], (1, 0, 2))

    if chosen is not None:
        start = 0
        for length in chosen:
            place = pl.ds(pl.multiple_of(pos_ref[at], RB), length)
            zn_out[:, start:start + length, :] = zn_ref[:, place, :]
            zkept[:, start:start + length, :] = zfull[:, place, :]
            start += length
            at += 1


def project(pieces, pos, mask, params, layer, sides, r0, r, total, chosen=None, z_out=False, keep=None, deps=()):
    scale, bias, w = params
    n = mask.shape[1]
    d = pieces[0][0].shape[2]
    parts, half2, ka = w.shape[2:]
    c = parts * half2 // 2
    blk = r0 // RB
    full = sides == 2
    b_shape, b_spec = jax.ShapeDtypeStruct((c, r, n), BF), pl.BlockSpec((c, RB, n), lambda i, pos: (0, i, 0))
    out_shape, out_specs = [b_shape], [b_spec]
    width = n if chosen is None else sum(chosen)
    if full:
        kept = 2 if z_out else 1
        out_shape = [jax.ShapeDtypeStruct((c, total, n), BF), b_shape] + [jax.ShapeDtypeStruct((total, width, d), BF)] * kept
        out_specs = [pl.BlockSpec((c, RB, n), lambda i, pos: (0, i + blk, 0)), b_spec] + [pl.BlockSpec((RB, width, d), lambda i, pos: (i + blk, 0, 0))] * kept
    scratch = [pltpu.VMEM((RB // 2, ka, 2 * n), BF), pltpu.VMEM((sides, RB, c, n), BF)]
    count = len(pieces)
    if count > 1 and not (z_out and chosen is None):
        scratch = scratch + [pltpu.VMEM((RB, n, d), BF)]
    if chosen is not None:
        scratch = scratch + [pltpu.VMEM((RB, n, d), BF)]
    keep = tuple(keep or ())
    extra = keep + tuple(deps)
    spec = pltpu.PrefetchScalarGridSpec(
        num_scalar_prefetch=1,
        grid=(r // RB,),
        in_specs=[pl.BlockSpec((RB, x.shape[1], d), functools.partial(lambda f, i, pos: (i + f, 0, 0), f // RB)) for x, f, _ in pieces]
        + [
            pl.BlockSpec((RB, n), lambda i, pos: (i + blk, 0)),
            pl.BlockSpec((None, d, LANES), lambda i, pos: (layer, 0, 0)),
            pl.BlockSpec((None, d, LANES), lambda i, pos: (layer, 0, 0)),
            pl.BlockSpec((None, sides) + w.shape[2:], lambda i, pos: (layer, 2 - sides, 0, 0, 0)),
        ]
        + [ANY] * len(extra),
        out_specs=out_specs,
        scratch_shapes=scratch,
    )
    first = 1 + count + 4
    return pl.pallas_call(
        functools.partial(proj_kernel, sides, [g for _, _, g in pieces], chosen, z_out, len(extra)),
        grid_spec=spec,
        out_shape=out_shape,
        name="project",
        input_output_aliases={first: 0, first + 1: 2, first + 2: 3} if keep else {},
        cost_estimate=pl.CostEstimate(flops=16 * sides * r * n * d * c, bytes_accessed=2 * r * n * d * (2 + sides), transcendentals=0),
        compiler_params=pltpu.CompilerParams(vmem_limit_bytes=VMEM),
    )(pos, *[x for x, _, _ in pieces], mask, scale, bias, w, *extra)


def tri_kernel(cb, layer, widths, spread, extra, pos_ref, *refs):
    count = len(widths)
    a_hbm, b_hbm, z_hbm, zn_hbm = refs[0], refs[1:1 + count], refs[1 + count], refs[2 + count]
    tail_hbm, refs = refs[3 + count:9 + count], refs[9 + count + extra:]
    o_ref, acc, on, a_ref, b_ref, z_ref, zn_ref = refs[:7]
    tail, (load_sem, z_sem, tail_sem) = refs[7:13], refs[13:]
    ls_ref, lb_ref, wo_ref, bo_ref, wg_ref, bg_ref = tail
    step = pl.program_id(0)
    c = acc.shape[0]
    width = sum(widths)
    starts = [sum(widths[:h]) for h in range(count)]

    @pl.when(step == 0)
    def _():
        loads = []
        for q in range(c // cb):
            ch = slice(q * cb, (q + 1) * cb)
            loads.append([pltpu.make_async_copy(a_hbm.at[ch], a_ref.at[ch], load_sem.at[q, count])])
            for h, wd in enumerate(widths):
                loads[q].append(pltpu.make_async_copy(b_hbm[h].at[ch], b_ref.at[ch, starts[h]:starts[h] + wd], load_sem.at[q, h]))
        later = []
        for k, (src, dst) in enumerate(zip(tail_hbm, tail)):
            later.append(pltpu.make_async_copy(src.at[layer], dst, tail_sem.at[k]))
        for h, wd in enumerate(widths):
            at, to = pl.ds(pl.multiple_of(pos_ref[h], RB), wd), slice(starts[h], starts[h] + wd)
            later.append(pltpu.make_async_copy(z_hbm.at[:, at], z_ref.at[:, to], z_sem.at[0, h]))
            later.append(pltpu.make_async_copy(zn_hbm.at[:, at], zn_ref.at[:, to], z_sem.at[1, h]))
        for copy in [x for group in loads for x in group] + later:
            copy.start()
        for q in range(c // cb):
            for copy in loads[q]:
                copy.wait()

            @pl.loop(q * cb, (q + 1) * cb, step=RB)
            def _(k0):
                for k in range(RB):
                    acc[k0 + k] = lax.dot_general(a_ref[k0 + k], b_ref[k0 + k], (((1,), (1,)), ((), ())), preferred_element_type=F32)

        for copy in later:
            copy.wait()

    ib = pl.multiple_of(step * RB, RB)
    zero = jnp.zeros((RB, width), F32)

    def block(k):
        return acc[pl.ds(pl.multiple_of(k * RB, RB), RB), pl.ds(ib, RB), :]

    mean = lax.fori_loop(0, c // RB, lambda k, t: t + jnp.sum(block(k), axis=0), zero) * (1.0 / c)

    def squares(k, t):
        v = block(k) - mean[None]
        return t + jnp.sum(v * v, axis=0)

    rstd = lax.rsqrt(lax.fori_loop(0, c // RB, squares, zero) * (1.0 / c) + LN_EPS)

    @pl.loop(0, c // RB)
    def _(k):
        k0 = pl.multiple_of(k * RB, RB)
        for t in range(0, width, LANES):
            sl = slice(t, min(t + LANES, width))
            v = acc[pl.ds(k0, RB), pl.ds(ib, RB), sl]
            lanes = sl.stop - sl.start
            v = (v - mean[None, :, sl]) * rstd[None, :, sl] * ls_ref[pl.ds(k0, RB), :, :lanes] + lb_ref[pl.ds(k0, RB), :, :lanes]
            on[:, pl.ds(k0, RB), sl] = jnp.transpose(v.astype(BF), (1, 0, 2))

    g_rows = ROWS_AT_ONCE if width <= LANES else ROWS_AT_ONCE // 2

    @pl.loop(0, RB, step=g_rows)
    def _(i0):
        rs = pl.ds(i0, g_rows)
        rows = pl.ds(ib + i0, g_rows)
        ont = jnp.transpose(on[rs], (0, 2, 1)).reshape(g_rows * width, c)
        u = jnp.dot(ont, wo_ref[...], preferred_element_type=F32) + bo_ref[...]
        u = u.astype(BF).astype(F32)
        g = jnp.dot(zn_ref[rows].reshape(g_rows * width, -1), wg_ref[...], preferred_element_type=F32) + bg_ref[...]
        new = z_ref[rows].astype(F32) + (jax.nn.sigmoid(g) * u).reshape(g_rows, width, -1)
        new = new.astype(BF)
        if spread:
            for h, wd in enumerate(widths):
                o_ref[rs, pl.ds(pl.multiple_of(pos_ref[h], RB), wd), :] = new[:, starts[h]:starts[h] + wd]
        else:
            o_ref[rs] = new


def triangle(pos, a, bs, z, zn, tail, layer, out_width=None, deps=()):
    c, r, n = a.shape
    d = z.shape[2]
    cb = CHANNELS
    widths = [b.shape[1] for b in bs]
    width = sum(widths)
    wide = out_width or width
    spec = pltpu.PrefetchScalarGridSpec(
        num_scalar_prefetch=1,
        grid=(r // RB,),
        in_specs=[ANY] * (3 + len(bs) + len(tail) + len(deps)),
        out_specs=pl.BlockSpec((RB, wide, d), lambda s, pos: (s, 0, 0)),
        scratch_shapes=[
            pltpu.VMEM((c, r, width), F32),
            pltpu.VMEM((RB, c, width), BF),
            pltpu.VMEM((c, r, n), BF),
            pltpu.VMEM((c, width, n), BF),
            pltpu.VMEM((r, width, d), BF),
            pltpu.VMEM((r, width, d), BF),
        ]
        + [pltpu.VMEM(x.shape[1:], x.dtype) for x in tail]
        + [pltpu.SemaphoreType.DMA((c // cb, 1 + len(bs))), pltpu.SemaphoreType.DMA((2, len(bs))), pltpu.SemaphoreType.DMA((len(tail),))],
    )
    return pl.pallas_call(
        functools.partial(tri_kernel, cb, layer, widths, out_width is not None, len(deps)),
        grid_spec=spec,
        out_shape=jax.ShapeDtypeStruct((r, wide, d), BF),
        name="triangle",
        cost_estimate=pl.CostEstimate(flops=16 * r * n * width * c, bytes_accessed=2 * c * n * (r + width), transcendentals=0),
        compiler_params=pltpu.CompilerParams(vmem_limit_bytes=VMEM),
    )(pos, a, *bs, z, zn, *tail, *deps)


def patch_kernel(pos_ref, piece_ref, whole_ref, out_ref):
    half = piece_ref.shape[1] // 2
    for h in range(2):
        out_ref[:, pl.ds(pl.multiple_of(pos_ref[1 + h], RB), half), :] = piece_ref[:, h * half:(h + 1) * half, :]


def patch(whole, piece, pos):
    r, j, d = piece.shape
    spec = pltpu.PrefetchScalarGridSpec(
        num_scalar_prefetch=1,
        grid=(r // RB,),
        in_specs=[pl.BlockSpec((RB, j, d), lambda i, pos: (i, 0, 0)), ANY],
        out_specs=pl.BlockSpec((RB, j, d), lambda i, pos: (i, pos[0], 0)),
    )
    return pl.pallas_call(
        patch_kernel,
        grid_spec=spec,
        out_shape=jax.ShapeDtypeStruct(whole.shape, BF),
        name="patch",
        input_output_aliases={2: 0},
    )(pos, piece, whole)


def side_weights(w_in, b_in):
    layers, d, c4 = w_in.shape
    w = jnp.transpose(w_in, (0, 2, 1))
    w = jnp.concatenate([w, b_in[:, :, None], jnp.zeros((layers, c4, 15), w_in.dtype)], axis=2) * 0.5
    w = w.reshape(layers, 2, 2, 2, c4 // 8, d + 16)
    return jnp.transpose(w, (0, 1, 3, 2, 4, 5)).reshape(layers, 2, 2, c4 // 4, d + 16)


def solution(mesh):
    row_spec = P(('batch', 'dap'), None, None)
    mask_spec = P(('batch', 'dap'), None)
    vec_spec = P(None, None)
    mat_spec = P(None, None, None)
    size = mesh.shape['dap']
    chips = size // 2
    side = [1 - 2 * (i % 2) for i in range(size)]
    to_helper = [(i, (i + 2 * side[i]) % size) for i in range(size)]
    to_other = [(i, (i - 2 * side[i]) % size) for i in range(size)]
    to_partner = [(i, i ^ 1) for i in range(size)]

    def device_fn(z_rows, mask_rows, ln_in_scale, ln_in_bias, w_in, b_in, w_gate, b_gate, ln_out_scale, ln_out_bias, w_out, b_out):
        def send(x, perm):
            return lax.ppermute(x, 'dap', perm)

        layers, d, _ = w_in.shape
        rows, n, _ = z_rows.shape
        lo = RB
        hi = rows - lo
        parts = ((0, hi), (hi, lo))
        index = lax.axis_index('dap')
        core, chip = index % 2, index // 2
        sgn = 1 - 2 * core

        def columns(segs, shift=0):
            at = [2 * rows * lax.rem(chip + (k + shift) * sgn + 4 * chips, chips) + rows * jnp.where(flip, 1 - core, core) + r0 for k, flip, r0, _ in segs]
            return jnp.stack(at).astype(jnp.int32)

        def lengths(segs):
            return [g[3] for g in segs]

        def whole(k):
            return [(k, flip, 0, rows) for flip in (0, 1)]

        mid = [[(k, flip, r0, r) for k in (1, -1) for flip in (0, 1)] for r0, r in parts]
        far_split = [(2, flip, r0, r) for r0, r in parts for flip in (0, 1)]

        z_hi = z_rows[:hi]
        near_in, other_in = [send(z_hi, to_helper)], [send(z_hi, to_other)]
        mask = mask_rows.astype(F32)
        mask_near, mask_other = send(mask, to_helper), send(mask, to_other)
        z_lo = z_rows[hi:]
        near_in.append(send(z_lo, to_helper))
        other_in.append(send(z_lo, to_other))

        scale = jnp.broadcast_to(ln_in_scale.astype(F32)[:, :, None], (layers, d, LANES))
        bias = jnp.broadcast_to(ln_in_bias.astype(F32)[:, :, None], (layers, d, LANES))
        params = (scale, bias, side_weights(w_in, b_in))
        c = ln_out_scale.shape[1]
        ls = jnp.broadcast_to(ln_out_scale.astype(F32)[:, :, None, None], (layers, c, 1, LANES))
        lb = jnp.broadcast_to(ln_out_bias.astype(F32)[:, :, None, None], (layers, c, 1, LANES))
        tail = (ls, lb, w_out, b_out.astype(F32)[:, None], w_gate, b_gate.astype(F32)[:, None])

        start = jnp.zeros((1,), jnp.int32)
        own_p, near_p, other_p, pos = None, None, None, None

        for layer in range(layers):
            final = layer + 1 == layers
            if layer == 0:
                far_segs = far_split
                a, b, zn = project([(z_rows, 0, [n])], start, mask, params, layer, 2, 0, rows, rows)
                b_p = send(b, to_partner)
                z_own = z_rows
                p0 = triangle(columns(whole(0)), a, [b, b_p], z_own, zn, tail, layer, None, (b,))
                p0_near, p0_other = send(p0, to_helper), send(p0, to_other)
                last = (p0,)
                near = None
                bn, bn_p, bo, bo_p = [None] * 2, [None] * 2, [None] * 2, [None] * 2
                for q, (r0, r) in enumerate(parts):
                    where = jnp.concatenate([start, columns(far_segs, -1)])
                    a_n, bn[q], zn_n, z_n = project([(near_in[q], 0, [n])], where, mask_near, params, layer, 2, r0, r, rows, lengths(far_segs), True, near, last)
                    near = (a_n, zn_n, z_n)
                    bn_p[q] = send(bn[q], to_partner)
                    bo[q], = project([(other_in[q], 0, [n])], start, mask_other, params, layer, 1, r0, r, rows, None, False, None, (bn[q],))
                    last = (bo[q],)
                    bo_p[q] = send(bo[q], to_partner)
                    if q == 0:
                        c1 = triangle(columns(mid[0]), a, [bo[0], bn_p[0], bn[0], bo_p[0]], z_own, zn, tail, layer, None, last)
                        last = (c1,)
                        c1_near = send(c1, to_helper)
                far_b = [bo[0], bn_p[0], bo[1], bn_p[1]]
            else:
                far_segs = whole(2)
                a, b, zn, z_own = project(own_p, pos[0], mask, params, layer, 2, 0, rows, rows, None, True, None, last)
                b_p = send(b, to_partner)
                where = jnp.concatenate([pos[1], columns(far_segs, -1)])
                a_n, bn, zn_n, z_n = project(near_p, where, mask_near, params, layer, 2, 0, rows, rows, lengths(far_segs), True, None, (b,))
                near = (a_n, zn_n, z_n)
                bn_p = send(bn, to_partner)
                bo, = project(other_p, pos[2], mask_other, params, layer, 1, 0, rows, rows, None, False, None, (bn,))
                bo_p = send(bo, to_partner)
                last = (bo,)
                far_b = [bo, bn_p]
            at, ends = 0, []
            for x in far_b:
                ends.append(at)
                at += x.shape[1]
            far = triangle(jnp.array(ends, jnp.int32), near[0], far_b, near[2], near[1], tail, layer, None, last)
            last = (far,)
            p3 = send(far, to_other)
            if layer == 0:
                c1_other = send(c1, to_other)
                c2 = triangle(columns(mid[1]), a, [bo[1], bn_p[1], bn[1], bo_p[1]], z_own, zn, tail, layer, None, last)
                last = (c2,)
                pieces = [(p0, whole(0)), (c1, mid[0]), (c2, mid[1])]
                near_got, other_got = [p0_near, c1_near, send(c2, to_helper)], [p0_other, c1_other, send(c2, to_other)]
            else:
                segs = whole(0) + whole(1) + whole(-1)
                rest = triangle(columns(segs), a, [b, b_p, bo, bn_p, bn, bo_p], z_own, zn, tail, layer, n if final else None, last)
                last = (rest,)
                if final:
                    block = lax.rem(chip + 2, chips)
                    return patch(rest, p3, jnp.stack([block, core * rows, (1 - core) * rows]).astype(jnp.int32))
                pieces = [(rest, segs)]
                near_got, other_got = [send(rest, to_helper)], [send(rest, to_other)]
            pieces.append((p3, far_segs))
            near_got.append(far)
            other_got.append(send(p3, to_other))
            every = [g for _, segs in pieces for g in segs]
            own_p = [(x, 0, lengths(segs)) for x, segs in pieces]
            near_p = [(x, 0, lengths(segs)) for x, (_, segs) in zip(near_got, pieces)]
            other_p = [(x, 0, lengths(segs)) for x, (_, segs) in zip(other_got, pieces)]
            pos = [columns(every), columns(every, -1), columns(every, 1)]

    return jax.shard_map(device_fn, mesh=mesh, in_specs=(row_spec, mask_spec, vec_spec, vec_spec, mat_spec, vec_spec, mat_spec, vec_spec, vec_spec, vec_spec, mat_spec, vec_spec), out_specs=row_spec, check_vma=False)
```
